32 devices in a mesh: section: 4 (over y, x), owner: 8 (over z, core).
Axes of the slice: x: 2, y: 2, z: 4, core: 2. Of those that a mesh axis runs over, the one named last changes fastest.
Arguments:
- weights: bfloat16 [4, 1024, 1024], P('section'), may hold values from -0.1875 to 0.1875
- inputs: bfloat16 [4, 4, 2048, 1024], P('section', None, 'owner'), may hold values from -6 to 6
- preact: bfloat16 [4, 4, 2048, 1024], P('section', None, 'owner'), may hold values from -6 to 6
- cotangent: bfloat16 [4, 2048, 1024], P(None, 'owner'), may hold values from -6 to 6
- embeddings: bfloat16 [4, 2048, 32, 128], P(None, ('owner', 'section')), may hold values from -6 to 6
- row_ids: int32 [4, 2048, 32], P(None, ('owner', 'section')), may hold values from 0 to 511
Outputs:
- weight_grad: float32 [4, 1024, 1024], P('section', 'owner')
- table_grad: float32 [32, 512, 128], P('owner', 'section')
The draws below stay inside these ranges and needn't reach their ends.
All inputs are finite; a program needn't handle non-finite values.
Results may differ from the reference program's by a relative error of at most 0.0064.
Values may be sent and summed in bfloat16 or wider, within the bound.
No kernel may reach another device: no remote copies, remote signals or barrier semaphores. Data moves between devices by JAX's collectives and lax.ppermute only.
A program may use at most 128 MiB of HBM per device.

```python
import math
import jax
import jax.numpy as jnp
import numpy as np
from jax import lax

F = 32
E = 128
H = 1024
MICRO = 4
TROWS = 512
LAYERS = 4
SLOTS = 32
ROWS = 512
BATCH = 2048


def with_ends(values, own_key, low, high):
    longest = values.shape.index(max(values.shape))
    spots = []
    for shift in (0, 1):
        where = [jax.random.randint(jax.random.fold_in(own_key, axis), (), 0, length) for axis, length in enumerate(values.shape)]
        where[longest] = (where[longest] + shift) % values.shape[longest]
        spots.append(tuple(where))
    return values.at[spots[0]].set(low).at[spots[1]].set(high)


def spiked(drawn, key, source, target, blocks, factor):
    def block_of(dim):
        return (jnp.arange(drawn.shape[dim]) // (drawn.shape[dim] // blocks)).reshape((-1,) + (1,) * (drawn.ndim - 1 - dim))

    near = jax.random.permutation(key, blocks)[block_of(target)]
    other_side = (block_of(target) + blocks // 2) % blocks
    return jnp.where((block_of(source) == near) | (block_of(source) == other_side), factor * drawn, drawn)


def shard_levels(key, extent, split, least, top_value):
    loudness = 1.0
    for dim, shards_of in split:
        draws = jax.random.uniform(jax.random.fold_in(jax.random.fold_in(key, 6), dim), (shards_of,), jnp.float32, least / len(split), top_value / len(split))
        loudness = loudness * jnp.repeat(jnp.exp(draws), extent[dim] // shards_of).reshape((-1,) + (1,) * (len(extent) - 1 - dim))
    return loudness


def rank_bounds(amount, skew):
    weights = [(1 << 20) // math.isqrt(standing ** skew) + 1 for standing in range(1, amount + 1)]
    deviation = 1 + sum(weights) // (1 << 30)
    return np.cumsum(np.array([max(1, weight // deviation) for weight in weights]))


def skewed_ids(stream_key, dims, number_of, skew):
    listing = rank_bounds(number_of, skew)
    ticket = jax.random.randint(jax.random.fold_in(stream_key, 1), dims, 0, int(listing[number_of - 1]))
    grade = jnp.searchsorted(jnp.asarray(listing, jnp.int32), ticket, side="right")
    return jax.random.permutation(jax.random.fold_in(stream_key, 2), number_of)[grade].astype(jnp.int32)


def gaussian(key, extent, width, limit, pieces=(), held_as=jnp.bfloat16):
    drawn = width * jax.random.normal(key, extent, jnp.float32)
    if pieces:
        drawn = drawn * shard_levels(key, extent, pieces, -0.22, 0.18)
    return jnp.clip(drawn, -limit, limit).astype(held_as)


def gaussian_with(rng, extent, spread, limit, pieces, heavy, kind=jnp.bfloat16):
    values = spread * jax.random.normal(rng, extent, jnp.float32)
    if pieces:
        values = values * shard_levels(rng, extent, pieces, -0.22, 0.18)
    return jnp.clip(spiked(values, jax.random.fold_in(rng, 3), *heavy), -limit, limit).astype(kind)


def setup_inputs(seed: int = 0) -> dict:
    arg_keys = jax.random.split(jax.random.key(seed), 7)
    return {
        "weights": gaussian(arg_keys[0], (LAYERS, H, H), H ** -0.5, 0.1875, ((0, 4),)),
        "inputs": gaussian_with(arg_keys[1], (LAYERS, MICRO, BATCH, H), 1.0, 6.0, ((0, 4), (2, 8)), (2, 3, 8, 2.0)),
        "preact": gaussian(arg_keys[2], (LAYERS, MICRO, BATCH, H), 1.0, 6.0, ((0, 4), (2, 8))),
        "cotangent": gaussian(arg_keys[3], (MICRO, BATCH, H), 1.0, 6.0, ((1, 8),)),
        "embeddings": gaussian(arg_keys[4], (MICRO, BATCH, F, E), 1.0, 6.0, ((1, 32),)),
        "row_ids": with_ends(skewed_ids(arg_keys[5], (MICRO, BATCH, F), ROWS, 2), jax.random.fold_in(arg_keys[5], 3), 0, ROWS - 1).astype(jnp.int32),
    }


def reference(weights, inputs, preact, cotangent, embeddings, row_ids):
    highest = lax.Precision.HIGHEST
    micro_count, sample_rows, hidden = cotangent.shape
    features = embeddings.shape[2]
    emb_width = embeddings.shape[3]
    grad_scale = 1.0 / math.sqrt(micro_count * sample_rows)
    upstream = cotangent
    layer_grads = []
    for layer_index in range(LAYERS - 1, -1, -1):
        slope = jnp.where(preact[layer_index] > 0, upstream, jnp.zeros_like(upstream))
        slope = slope.reshape(micro_count * sample_rows, hidden)
        flat_in = inputs[layer_index].reshape(micro_count * sample_rows, hidden)
        layer_grads.append(jnp.dot(flat_in.T.astype(jnp.float32), slope.astype(jnp.float32), precision=highest) * grad_scale)
        upstream = jnp.dot(slope.astype(jnp.float32), weights[layer_index].T.astype(jnp.float32), precision=highest)
        upstream = upstream.astype(jnp.bfloat16).reshape(micro_count, sample_rows, hidden)
    weight_grad = jnp.stack(layer_grads[::-1])

    def feature_grads(members):
        flat_grad, embedded = members
        square = flat_grad.reshape(sample_rows, features, features).astype(jnp.float32)
        emb32 = embedded.astype(jnp.float32)
        direct = jnp.einsum('qfg,qge->qfe', square, emb32, precision=highest)
        swapped = jnp.einsum('qgf,qge->qfe', square, emb32, precision=highest)
        return (direct + swapped).astype(jnp.bfloat16)
    grads_all = lax.map(feature_grads, (upstream, embeddings))
    flat_grads = grads_all.reshape(micro_count * sample_rows, features, emb_width)
    flat_ids = row_ids.reshape(micro_count * sample_rows, features)

    def one_table(feature_index):
        column = lax.dynamic_index_in_dim(flat_grads, feature_index, 1, False).astype(jnp.float32)
        row_index = lax.dynamic_index_in_dim(flat_ids, feature_index, 1, False)
        return jax.ops.segment_sum(column, row_index, num_segments=ROWS)
    tables = lax.map(one_table, jnp.arange(features, dtype=jnp.int32))
    table_grad = (tables * grad_scale).reshape(SLOTS, TROWS, emb_width)
    return (weight_grad, table_grad)
```

```python
import functools
import math

import jax
import jax.numpy as jnp
from jax import lax
from jax.experimental import pallas as pl
from jax.experimental.pallas import tpu as pltpu
from jax.sharding import Mesh, PartitionSpec as P

TROWS = 512
STREAMS = 2
GROUPS = 2
IDS_SLOT = 3


def pair_grads(flat_grad, embedded, features):
    sample_count = flat_grad.shape[0]
    square = flat_grad.reshape(sample_count, features, features)
    direct = jnp.einsum("qfg,qge->fqe", square, embedded, preferred_element_type=jnp.float32)
    swapped = jnp.einsum("qgf,qge->fqe", square, embedded, preferred_element_type=jnp.float32)
    return (direct + swapped).astype(jnp.bfloat16)


def row_sums_body(ids_ref, arrived_ref, *rest, sources, rows):
    acc_ref = rest[0] if len(rest) == 2 else None
    out_ref = rest[-1]
    width = arrived_ref.shape[2]
    step = 2 if sources % 2 == 0 else 1
    total = None
    for source in range(0, sources, step):
        hot = []
        for one in range(source, source + step):
            places = ids_ref[0, one : one + 1, :]
            marks = lax.broadcasted_iota(jnp.int32, (rows, width), 0) == places
            hot.append(marks.astype(jnp.float32).astype(jnp.bfloat16))
        left = jnp.concatenate(hot, axis=1)
        right = arrived_ref[source : source + step, 0].reshape(step * width, -1)
        part = jnp.dot(left, right, preferred_element_type=jnp.float32)
        total = part if total is None else total + part
    if acc_ref is not None:
        total = total + acc_ref[0]
    out_ref[0] = total


def row_sums(ids, arrived, running, rows):
    sources, slots, width, emb = arrived.shape
    in_specs = [
        pl.BlockSpec((1, sources, width), lambda s: (s, 0, 0)),
        pl.BlockSpec((sources, 1, width, emb), lambda s: (0, s, 0, 0)),
    ]
    args = [ids, arrived]
    if running is not None:
        in_specs.append(pl.BlockSpec((1, rows, emb), lambda s: (s, 0, 0)))
        args.append(running)
    return pl.pallas_call(
        functools.partial(row_sums_body, sources=sources, rows=rows),
        grid=(slots,),
        in_specs=in_specs,
        out_specs=pl.BlockSpec((1, rows, emb), lambda s: (s, 0, 0)),
        out_shape=jax.ShapeDtypeStruct((slots, rows, emb), jnp.float32),
        cost_estimate=pl.CostEstimate(
            flops=2 * slots * rows * sources * width * emb,
            bytes_accessed=arrived.size * 2 + slots * rows * emb * 8,
            transcendentals=0,
        ),
        name="row_sums",
    )(*args)


def weight_half_body(where_ref, *rest, stacks, shifts, chunk_count, sections):
    in_refs = rest[:stacks]
    slope_refs = rest[stacks:-3]
    out_ref, held, sems = rest[-3:]
    section = where_ref[0]
    for pos, shift in enumerate(shifts):

        @pl.when(section == pos)
        def _():
            for chunk in range(chunk_count):
                pltpu.make_async_copy(
                    slope_refs[chunk + shift], held.at[chunk], sems.at[chunk]
                ).start()

    total = None
    for chunk in range(0, chunk_count, 2):
        left = []
        for one in (chunk, chunk + 1):
            pltpu.make_async_copy(slope_refs[one], held.at[one], sems.at[one]).wait()
            group, quarter = one // sections, sections - 1 - one % sections
            left.append(
                jnp.concatenate(
                    [ref[group, :, quarter].reshape(-1, ref.shape[-1]) for ref in in_refs],
                    axis=1,
                )
            )
        left = jnp.concatenate(left, axis=0)
        right = held[chunk : chunk + 2].reshape(left.shape[0], -1)
        part = lax.dot_general(
            left, right, (((0,), (0,)), ((), ())), preferred_element_type=jnp.float32
        )
        total = part if total is None else total + part
    out_ref[...] = total.astype(out_ref.dtype)


def weight_half(where, layer_in, slopes, shifts, stacks, cores, dtype):
    groups, _, sections, _, hidden = layer_in.shape
    unit = hidden // (stacks * cores)
    chunk_rows = slopes[0].shape[0]
    chunk_count = groups * sections
    lead = layer_in.shape[:-1]

    def block(stack):
        return pl.BlockSpec(
            lead + (unit,), lambda i, where: (0, 0, 0, 0, stack * cores + where[1])
        )

    grid_spec = pltpu.PrefetchScalarGridSpec(
        num_scalar_prefetch=1,
        grid=(1,),
        in_specs=[block(stack) for stack in range(stacks)]
        + [pl.BlockSpec(memory_space=pl.ANY)] * len(slopes),
        out_specs=pl.BlockSpec((stacks * unit, hidden), lambda i, where: (0, 0)),
        scratch_shapes=[
            pltpu.VMEM((chunk_count, chunk_rows, hidden), jnp.bfloat16),
            pltpu.SemaphoreType.DMA((chunk_count,)),
        ],
    )
    return pl.pallas_call(
        functools.partial(
            weight_half_body,
            stacks=stacks,
            shifts=shifts,
            chunk_count=chunk_count,
            sections=sections,
        ),
        grid_spec=grid_spec,
        out_shape=jax.ShapeDtypeStruct((stacks * unit, hidden), dtype),
        cost_estimate=pl.CostEstimate(
            flops=2 * layer_in.size * unit * stacks,
            bytes_accessed=layer_in.size * 4,
            transcendentals=0,
        ),
        name="weight_half",
    )(where, *([layer_in] * stacks), *slopes)


def exchange(blocks, axis):
    size = lax.axis_size(axis)
    place = lax.axis_index(axis)
    if size > 8:
        came = lax.all_to_all(
            blocks.astype(jnp.bfloat16), axis, split_axis=0, concat_axis=0, tiled=True
        )
        return jnp.sum(came.astype(jnp.float32), axis=0)
    total = lax.dynamic_index_in_dim(blocks, place, 0, False)
    for shift in range(1, size):
        sent = lax.dynamic_index_in_dim(blocks, (place + shift) % size, 0, False)
        turn = [(i, (i + shift) % size) for i in range(size)]
        came = lax.ppermute(sent.astype(jnp.bfloat16), axis, turn)
        total = total + came.astype(jnp.float32)
    return total


def per_device(weights, inputs, preact, cotangent, embeddings, row_ids):
    sections = lax.axis_size("section")
    stacks = lax.axis_size("stack")
    cores = lax.axis_size("core")
    owners = stacks * cores
    section_pos = lax.axis_index("section")
    core_pos = lax.axis_index("core")
    owner_pos = lax.axis_index("stack") * cores + core_pos
    micro_count, batch_rows, hidden = cotangent.shape
    features = embeddings.shape[2]
    emb_width = embeddings.shape[3]
    quarter = batch_rows // sections
    row_split = max(1, owners // features)
    slot_count = features * row_split // owners
    first_slot = owner_pos * slot_count
    grad_scale = 1.0 / math.sqrt(micro_count * batch_rows * owners)
    last = sections - 1
    is_last = section_pos == last
    layer_w = weights[0]

    in_group = micro_count // GROUPS
    order = list(range(last, -1, -1))
    chunk_count = GROUPS * sections
    chunk_rows = in_group * quarter
    view = (GROUPS, in_group, sections, quarter, hidden)
    cot_view = cotangent.reshape(view)
    pre_view = preact[0].reshape(view)

    down = [(i, i - 1) for i in range(1, sections)]
    fill = STREAMS * last
    total_slots = chunk_count + fill
    shifts = [STREAMS * (last - pos) for pos in range(sections)]
    shift_now = STREAMS * (last - section_pos)
    received = {}
    slopes = []
    pieces = {}
    table = None
    for slot in range(total_slots):
        spot = jnp.clip(slot - shift_now, 0, chunk_count - 1)
        zero = jnp.zeros_like(spot)
        pre_now = lax.dynamic_slice(
            pre_view,
            (lax.div(spot, sections), zero, last - lax.rem(spot, sections), zero, zero),
            (1, in_group, 1, quarter, hidden),
        ).reshape(chunk_rows, hidden)
        if slot < chunk_count:
            incoming = cot_view[slot // sections, :, order[slot % sections]]
            incoming = incoming.reshape(chunk_rows, hidden)
            if slot >= STREAMS:
                incoming = jnp.where(is_last, incoming, received.pop(slot - STREAMS))
        else:
            incoming = received.pop(slot - STREAMS)
        slope = jnp.where(pre_now > 0, incoming, jnp.zeros_like(incoming))
        slopes.append(slope)
        passed = lax.dot_general(
            slope, layer_w, (((1,), (1,)), ((), ())), preferred_element_type=jnp.float32
        ).astype(jnp.bfloat16)
        chunk = slot - fill
        target = order[chunk % sections] if chunk >= 0 else None
        if slot == IDS_SLOT:
            ids, passed = lax.optimization_barrier((row_ids, passed))
            ids = jnp.transpose(ids, (2, 0, 1)).reshape(features, micro_count * quarter)
            ids = lax.all_to_all(
                jnp.repeat(ids, row_split, axis=0),
                ("stack", "core"),
                split_axis=0,
                concat_axis=0,
                tiled=True,
            )
            slot_ids = first_slot + jnp.arange(slot_count, dtype=jnp.int32)
            ids = ids.reshape(owners, slot_count, micro_count * quarter)
            ids = ids - ((slot_ids % row_split) * TROWS)[None, :, None]
            ids = jnp.transpose(ids, (1, 0, 2))
        if slot < total_slots - STREAMS:
            pairs = down + [(0, last)] if target == last else down
            received[slot] = lax.ppermute(passed, "section", pairs)
        if chunk < 0:
            continue
        group = chunk // sections
        if target == 0:
            pieces[0] = passed
        elif target == last and slot in received:
            pieces[last] = received[slot]
        else:
            pieces[target] = lax.ppermute(passed, "section", [(0, target)])
        if len(pieces) == sections:
            mine = pieces.pop(0)
            for key in list(pieces):
                mine = jnp.where(section_pos == key, pieces.pop(key), mine)
            embedded = embeddings[group * in_group : (group + 1) * in_group]
            feat = pair_grads(
                mine, embedded.reshape(chunk_rows, features, emb_width), features
            )
            arrived = lax.all_to_all(
                jnp.repeat(feat, row_split, axis=0),
                ("stack", "core"),
                split_axis=0,
                concat_axis=0,
                tiled=True,
            )
            arrived = arrived.reshape(owners, slot_count, chunk_rows, emb_width)
            ids_now = ids[:, :, group * chunk_rows : (group + 1) * chunk_rows]
            table = row_sums(ids_now, arrived, table, TROWS)

    unit = hidden // owners
    halves = []
    if unit % 128 == 0:
        in_view = inputs[0].reshape(view)
        for shift in range(cores - 1, -1, -1):
            where = jnp.stack([section_pos, (core_pos + shift) % cores]).astype(jnp.int32)
            dtype = jnp.bfloat16 if shift else jnp.float32
            halves.append(
                weight_half(where, in_view, slopes, shifts, stacks, cores, dtype)
            )
    else:
        line = jnp.concatenate(slopes, 0)
        flat_slope = lax.dynamic_slice_in_dim(
            line,
            STREAMS * (last - section_pos) * chunk_rows,
            micro_count * batch_rows,
            0,
        )
        in_order = inputs[0].reshape(view)[:, :, jnp.asarray(order)]
        in_order = jnp.swapaxes(in_order, 1, 2).reshape(micro_count * batch_rows, hidden)
        full = lax.dot_general(
            in_order, flat_slope, (((0,), (0,)), ((), ())), preferred_element_type=jnp.float32
        ).reshape(stacks, cores, unit, hidden)
        for shift in range(cores - 1, -1, -1):
            side = lax.dynamic_index_in_dim(full, (core_pos + shift) % cores, 1, False)
            side = side.reshape(stacks * unit, hidden)
            halves.append(side.astype(jnp.bfloat16) if shift else side)
    summed = halves[-1]
    for place in range(cores - 1):
        shift = cores - 1 - place
        turn = [(i, (i + shift) % cores) for i in range(cores)]
        summed = summed + lax.ppermute(halves[place], "core", turn).astype(jnp.float32)
    weight_grad = exchange(summed.reshape(stacks, unit, hidden), "stack") * grad_scale

    shared = table.reshape(slot_count, sections, TROWS // sections, emb_width)
    table_grad = exchange(jnp.swapaxes(shared, 0, 1), "section") * grad_scale
    return (weight_grad[None], table_grad)


def solution(mesh):
    sections, owners = mesh.devices.shape
    cores = 2 if owners % 2 == 0 else 1
    inner = Mesh(
        mesh.devices.reshape(sections, owners // cores, cores), ("section", "stack", "core")
    )
    own = ("stack", "core")
    return jax.shard_map(
        per_device,
        mesh=inner,
        in_specs=(
            P("section", None, None),
            P("section", None, own, None),
            P("section", None, own, None),
            P(None, own, None),
            P(None, ("stack", "core", "section"), None, None),
            P(None, ("stack", "core", "section"), None),
        ),
        out_specs=(P("section", own, None), P(own, "section", None)),
        check_vma=False,
    )
```

```python
import functools
import math

import jax
import jax.numpy as jnp
from jax import lax
from jax.experimental import pallas as pl
from jax.experimental.pallas import tpu as pltpu
from jax.sharding import Mesh, PartitionSpec as P


TROWS = 512
STREAMS = 2
GROUPS = 2
NEAR_SLOTS = 4


def pair_body(where_ref, *rest, features, per_far, group_size, row_split, marks):
    piece_refs, emb_ref = rest[: len(marks)], rest[len(marks)]
    out_refs, held = rest[len(marks) + 1 : -1], rest[-1]
    flat = piece_refs[0][...]
    for mark, ref in zip(marks[1:], piece_refs[1:]):
        flat = jnp.where(where_ref[0] == mark, ref[...], flat)
    square = flat.reshape(flat.shape[0], features, features).astype(jnp.float32)
    both = (square + jnp.swapaxes(square, 1, 2)).astype(jnp.bfloat16)
    grads = lax.dot_general(
        both, emb_ref[0], (((2,), (1,)), ((0,), (0,))), preferred_element_type=jnp.float32
    ).astype(jnp.bfloat16)
    held[...] = jnp.swapaxes(grads, 0, 1)
    for turn, out_ref in enumerate(out_refs):
        for place in range(out_ref.shape[0]):
            far, rest_of = place // per_far, place % per_far
            slot = (far * group_size + where_ref[1 + turn]) * per_far + rest_of
            out_ref[place] = held[lax.div(slot, row_split)]


def pair_grads(where, pieces, marks, embeddings, group, slots, per_far, group_size, row_split):
    _, rows, features, emb_width = embeddings.shape
    samples, hidden = pieces[0].shape
    steps = samples // rows
    count = slots // group_size
    shape = jax.ShapeDtypeStruct((count, samples, emb_width), jnp.bfloat16)
    grid_spec = pltpu.PrefetchScalarGridSpec(
        num_scalar_prefetch=1,
        grid=(steps,),
        in_specs=[pl.BlockSpec((rows, hidden), lambda i, where: (i, 0))] * len(pieces)
        + [
            pl.BlockSpec(
                (1, rows, features, emb_width), lambda i, where: (group * steps + i, 0, 0, 0)
            )
        ],
        out_specs=[pl.BlockSpec((count, rows, emb_width), lambda i, where: (0, i, 0))]
        * group_size,
        scratch_shapes=[pltpu.VMEM((features, rows, emb_width), jnp.bfloat16)],
    )
    return pl.pallas_call(
        functools.partial(
            pair_body,
            features=features,
            per_far=per_far,
            group_size=group_size,
            row_split=row_split,
            marks=marks,
        ),
        grid_spec=grid_spec,
        out_shape=[shape] * group_size,
        compiler_params=pltpu.CompilerParams(vmem_limit_bytes=24 * 2**20),
        cost_estimate=pl.CostEstimate(
            flops=16 * samples * features * features * emb_width,
            bytes_accessed=samples * (features * emb_width * 4 + hidden * 8),
            transcendentals=0,
        ),
        name="pair_grads",
    )(where, *pieces, embeddings)


def row_sums_body(ids_ref, *rest, rows):
    arrived_refs, out_ref = rest[:-1], rest[-1]
    width = arrived_refs[0].shape[1]
    sources = len(arrived_refs)
    step = 2 if sources % 2 == 0 else 1
    positions = lax.broadcasted_iota(jnp.int32, (rows, step * width), 0)
    total = None
    for source in range(0, sources, step):
        places = ids_ref[0, :, source * width : (source + step) * width]
        left = jnp.where(positions == places, 1.0, 0.0).astype(jnp.bfloat16)
        right = jnp.concatenate([arrived_refs[source + i][0] for i in range(step)], axis=0)
        part = jnp.dot(left, right, preferred_element_type=jnp.float32)
        total = part if total is None else total + part
    out_ref[:, 0] = total.astype(out_ref.dtype).reshape(out_ref.shape[0], -1, total.shape[1])


def row_sums(ids, arrived, rows, parts):
    slots, width, emb = arrived[0].shape
    sources = len(arrived)
    in_specs = [pl.BlockSpec((1, 1, sources * width), lambda s: (s, 0, 0))]
    in_specs += [pl.BlockSpec((1, width, emb), lambda s: (s, 0, 0))] * sources
    return pl.pallas_call(
        functools.partial(row_sums_body, rows=rows),
        grid=(slots,),
        in_specs=in_specs,
        out_specs=pl.BlockSpec((parts, 1, rows // parts, emb), lambda s: (0, s, 0, 0)),
        out_shape=jax.ShapeDtypeStruct((parts, slots, rows // parts, emb), jnp.bfloat16),
        compiler_params=pltpu.CompilerParams(vmem_limit_bytes=16 * 2**20),
        cost_estimate=pl.CostEstimate(
            flops=2 * slots * rows * sources * width * emb,
            bytes_accessed=sources * slots * width * emb * 2 + slots * rows * emb * 2,
            transcendentals=0,
        ),
        name="row_sums",
    )(ids, *arrived)


def flip_body(in_ref, out_ref):
    block = in_ref[0, :, 0]
    out_ref[...] = block.reshape(-1, block.shape[-1]).T


def flip(layer_in):
    groups, in_group, sections, rows, hidden = layer_in.shape
    chunk_count = groups * sections
    return pl.pallas_call(
        flip_body,
        grid=(chunk_count,),
        in_specs=[
            pl.BlockSpec(
                (1, in_group, 1, rows, hidden),
                lambda c: (c // sections, 0, sections - 1 - c % sections, 0, 0),
            )
        ],
        out_specs=pl.BlockSpec((hidden, in_group * rows), lambda c: (0, c)),
        out_shape=jax.ShapeDtypeStruct(
            (hidden, chunk_count * in_group * rows), layer_in.dtype
        ),
        cost_estimate=pl.CostEstimate(
            flops=2 * layer_in.size * 256, bytes_accessed=layer_in.size * 4, transcendentals=0
        ),
        compiler_params=pltpu.CompilerParams(vmem_limit_bytes=16 * 2**20),
        name="flip",
    )(layer_in)


def weight_half_body(where_ref, flipped_ref, *rest, slots, far_slots, shifts, spots, merged):
    slope_refs = rest[:slots]
    came_ref = rest[slots] if merged else None
    out_refs, left, held, sems = rest[slots + merged : -3], rest[-3], rest[-2], rest[-1]
    section = where_ref[0]
    chunk_count = held.shape[0]
    stacks, unit, _ = left.shape
    blocks = []
    for turn in range(stacks):
        stack = spots(where_ref[2], turn)
        row = pl.multiple_of((stack * where_ref[3] + where_ref[1]) * unit, unit)
        blocks.append(
            pltpu.make_async_copy(
                flipped_ref.at[pl.ds(row, unit), :], left.at[turn], sems.at[chunk_count + turn]
            )
        )
    for copy in blocks:
        copy.start()
    for pos, shift in enumerate(shifts):

        @pl.when(section == pos)
        def _():
            copies = [
                pltpu.make_async_copy(slope_refs[chunk + shift], held.at[chunk], sems.at[chunk])
                for chunk in range(chunk_count)
                if chunk + shift < far_slots
            ]
            for copy in copies:
                copy.start()
            for chunk in range(len(copies), chunk_count):
                held[chunk] = slope_refs[chunk + shift][...]
            for copy in copies:
                copy.wait()

    for copy in blocks:
        copy.wait()
    right = held[...].reshape(left.shape[2], -1)
    total = jnp.dot(
        left[...].reshape(stacks * unit, -1), right, preferred_element_type=jnp.float32
    )
    if merged:
        parts = []
        for turn in range(stacks):
            row = pl.multiple_of(spots(where_ref[2], turn) * unit, unit)
            parts.append(came_ref[pl.ds(row, unit), :].astype(jnp.float32))
        total = total + jnp.concatenate(parts, axis=0)
    done = 0
    for out_ref in out_refs:
        rows = out_ref.shape[0]
        out_ref[...] = total[done : done + rows].astype(out_ref.dtype)
        done += rows


def weight_half(where, flipped, slopes, shifts, stacks, spots, came=None):
    hidden = slopes[0].shape[1]
    chunk_rows = slopes[0].shape[0]
    chunk_count = flipped.shape[1] // chunk_rows
    rows = flipped.shape[0] // 2
    unit = rows // stacks
    far_slots = len(slopes) - NEAR_SLOTS
    in_specs = [pl.BlockSpec(memory_space=pl.ANY)] * (1 + far_slots)
    in_specs += [pl.BlockSpec(memory_space=pltpu.VMEM)] * NEAR_SLOTS
    args = [flipped] + list(slopes)
    if came is None:
        shapes = [jax.ShapeDtypeStruct((rows, hidden), jnp.bfloat16)]
    else:
        in_specs.append(pl.BlockSpec(came.shape, lambda i, where: (0, 0)))
        args.append(came)
        shapes = [
            jax.ShapeDtypeStruct((unit, hidden), jnp.float32),
            jax.ShapeDtypeStruct((unit, hidden), jnp.float32),
            jax.ShapeDtypeStruct((2 * unit, hidden), jnp.bfloat16),
        ]
    grid_spec = pltpu.PrefetchScalarGridSpec(
        num_scalar_prefetch=1,
        grid=(1,),
        in_specs=in_specs,
        out_specs=[pl.BlockSpec(shape.shape, lambda i, where: (0, 0)) for shape in shapes],
        scratch_shapes=[
            pltpu.VMEM((stacks, unit, flipped.shape[1]), jnp.bfloat16),
            pltpu.VMEM((chunk_count, chunk_rows, hidden), jnp.bfloat16),
            pltpu.SemaphoreType.DMA((chunk_count + stacks,)),
        ],
    )
    return pl.pallas_call(
        functools.partial(
            weight_half_body,
            slots=len(slopes),
            far_slots=far_slots,
            shifts=shifts,
            spots=spots,
            merged=came is not None,
        ),
        grid_spec=grid_spec,
        out_shape=shapes,
        compiler_params=pltpu.CompilerParams(vmem_limit_bytes=24 * 2**20),
        cost_estimate=pl.CostEstimate(
            flops=flipped.size * hidden, bytes_accessed=flipped.size * 6, transcendentals=0
        ),
        name="weight_half",
    )(where, *args)


def natural(stack, turn):
    return turn


def from_own(stack, turn):
    return ((stack // 2) ^ (turn % 2)) * 2 + ((stack % 2) ^ (turn // 2))


def exchange(blocks, axis):
    size = lax.axis_size(axis)
    place = lax.axis_index(axis)
    if size > 8:
        came = lax.all_to_all(
            blocks.astype(jnp.bfloat16), axis, split_axis=0, concat_axis=0, tiled=True
        )
        return jnp.sum(came.astype(jnp.float32), axis=0)
    total = lax.dynamic_index_in_dim(blocks, place, 0, False).astype(jnp.float32)
    for shift in range(1, size):
        sent = lax.dynamic_index_in_dim(blocks, (place + shift) % size, 0, False)
        turn = [(i, (i + shift) % size) for i in range(size)]
        came = lax.ppermute(sent.astype(jnp.bfloat16), axis, turn)
        total = total + came.astype(jnp.float32)
    return total


def after(value, *others):
    return lax.optimization_barrier((value,) + others)[0]


def per_device(weights, inputs, preact, cotangent, embeddings, row_ids):
    sections = lax.axis_size("section")
    fars = lax.axis_size("far")
    nears = lax.axis_size("near")
    stacks = fars * nears
    cores = lax.axis_size("core")
    owners = stacks * cores
    section_pos = lax.axis_index("section")
    core_pos = lax.axis_index("core")
    stack_pos = lax.axis_index("far") * nears + lax.axis_index("near")
    micro_count, batch_rows, hidden = cotangent.shape
    features = embeddings.shape[2]
    emb_width = embeddings.shape[3]
    quarter = batch_rows // sections
    row_split = max(1, owners // features)
    slot_count = features * row_split // owners
    grad_scale = 1.0 / math.sqrt(micro_count * batch_rows * owners)
    last = sections - 1
    is_last = section_pos == last
    layer_w = weights[0]

    in_group = micro_count // GROUPS
    order = list(range(last, -1, -1))
    chunk_count = GROUPS * sections
    chunk_rows = in_group * quarter
    view = (GROUPS, in_group, sections, quarter, hidden)
    cot_view = cotangent.reshape(view)
    pre_view = preact[0].reshape(view)

    down = [(i, i - 1) for i in range(1, sections)]
    fill = STREAMS * last
    total_slots = chunk_count + fill
    shifts = [STREAMS * (last - pos) for pos in range(sections)]
    shift_now = STREAMS * (last - section_pos)
    unit = hidden // owners
    in_view = inputs[0].reshape(view)
    flipped = None
    group_size = nears * cores
    near_core = lax.axis_index("near") * cores + core_pos
    held_slots = (
        jnp.arange(fars, dtype=jnp.int32)[:, None] * (group_size * slot_count)
        + near_core * slot_count
        + jnp.arange(slot_count, dtype=jnp.int32)[None, :]
    ).reshape(fars * slot_count)

    partners = [near_core]
    ways = [None]
    for turn in range(1, group_size):
        flip_near, flip_core = turn // cores, turn % cores
        near, core = near_core // cores, near_core % cores
        partners.append((near ^ flip_near) * cores + (core ^ flip_core))
        ways.append(
            [
                (i, (i // cores ^ flip_near) * cores + (i % cores ^ flip_core))
                for i in range(group_size)
            ]
        )

    def to_holders(blocks):
        came = [blocks[0]]
        for turn in range(1, group_size):
            came.append(lax.ppermute(blocks[turn], ("near", "core"), ways[turn]))
        return came

    received = {}
    slopes = []
    pieces = {}
    waiting = []
    arrived = []
    ids = None
    for slot in range(total_slots):
        spot = jnp.clip(slot - shift_now, 0, chunk_count - 1)
        zero = jnp.zeros_like(spot)
        if slot >= 2 * STREAMS and slot % STREAMS == 0:
            pre_view = after(pre_view, passed)
        pre_now = lax.dynamic_slice(
            pre_view,
            (lax.div(spot, sections), zero, last - lax.rem(spot, sections), zero, zero),
            (1, in_group, 1, quarter, hidden),
        ).reshape(chunk_rows, hidden)
        if slot < chunk_count:
            incoming = cot_view[slot // sections, :, order[slot % sections]]
            incoming = incoming.reshape(chunk_rows, hidden)
            if slot >= STREAMS:
                incoming = jnp.where(is_last, incoming, received.pop(slot - STREAMS))
        else:
            incoming = received.pop(slot - STREAMS)
        slope = jnp.where(pre_now > 0, incoming, jnp.zeros_like(incoming))
        slopes.append(slope)
        passed = lax.dot_general(
            slope, layer_w, (((1,), (1,)), ((), ())), preferred_element_type=jnp.float32
        ).astype(jnp.bfloat16)
        chunk = slot - fill
        target = order[chunk % sections] if chunk >= 0 else None
        in_chain = slot < total_slots - STREAMS
        if in_chain:
            pairs = down + [(0, last)] if target == last else down
            received[slot] = lax.ppermute(passed, "section", pairs)
        if chunk >= 0:
            if target == last and in_chain:
                pieces[chunk] = received[slot]
            elif target == 0:
                pieces[chunk] = passed
            else:
                waiting.append((chunk, target, slot, passed))
        if in_chain and slot % STREAMS != STREAMS - 1:
            continue
        if ids is None and slot > STREAMS:
            ids = jnp.transpose(after(row_ids, passed), (2, 0, 1))
            ids = jnp.repeat(ids.reshape(features, micro_count * quarter), row_split, axis=0)
            ids = ids.reshape(fars, group_size, slot_count, micro_count * quarter)
            ids = [
                lax.dynamic_index_in_dim(ids, partner, 1, False).reshape(
                    fars * slot_count, micro_count * quarter
                )
                for partner in partners
            ]
            ids = to_holders(ids)
            ids = jnp.concatenate(
                [
                    source[:, group * chunk_rows : (group + 1) * chunk_rows]
                    for group in range(GROUPS)
                    for source in ids
                ],
                axis=1,
            )
            if row_split > 1:
                ids = ids - ((held_slots % row_split) * TROWS)[:, None]
            ids = ids[:, None, :]
        elif ids is not None and flipped is None and unit % 128 == 0 and fars == nears == cores == 2:
            flipped = flip(after(in_view, passed))
        ready = None
        if chunk >= 0:
            group = chunk // sections - (0 if chunk % sections == last else 1)
            if group >= 0 and all(group * sections + q in pieces for q in range(sections)):
                ready = group
        for sent, target, sent_slot, held in waiting:
            pieces[sent] = lax.ppermute(after(held, passed), "section", [(0, target)])
        waiting = []
        final = chunk == chunk_count - 1
        if final:
            ready = GROUPS - 1
        if ready is None:
            continue
        ready_pieces = [pieces.pop(ready * sections + q) for q in range(sections)]
        where = jnp.stack([section_pos] + partners).astype(jnp.int32)
        blocks = pair_grads(
            where,
            ready_pieces,
            order,
            embeddings,
            ready,
            features * row_split,
            slot_count,
            group_size,
            row_split,
        )
        arrived.append(to_holders(blocks))

    if flipped is not None:
        where = jnp.stack(
            [section_pos, 1 - core_pos, stack_pos, jnp.full_like(section_pos, cores)]
        ).astype(jnp.int32)
        (side,) = weight_half(where, flipped, slopes, shifts, stacks, natural)
        came = lax.ppermute(side, "core", [(0, 1), (1, 0)])
        where = jnp.stack(
            [section_pos, core_pos, stack_pos, jnp.full_like(section_pos, cores)]
        ).astype(jnp.int32)
        own_rows, far_rows, near_rows = weight_half(
            where, flipped, slopes, shifts, stacks, from_own, came
        )
        near_came = lax.ppermute(near_rows, "near", [(0, 1), (1, 0)]).astype(jnp.float32)
    table = row_sums(ids, [block for group in arrived for block in group], TROWS, sections)

    if flipped is not None:
        far_sum = (far_rows + near_came[unit:]).astype(jnp.bfloat16)
        far_came = lax.ppermute(far_sum, "far", [(0, 1), (1, 0)]).astype(jnp.float32)
        weight_grad = (own_rows + near_came[:unit] + far_came) * grad_scale
    else:
        line = jnp.concatenate(slopes, 0)
        flat_slope = lax.dynamic_slice_in_dim(
            line,
            STREAMS * (last - section_pos) * chunk_rows,
            micro_count * batch_rows,
            0,
        )
        in_order = in_view[:, :, jnp.asarray(order)]
        in_order = jnp.swapaxes(in_order, 1, 2).reshape(micro_count * batch_rows, hidden)
        full = lax.dot_general(
            in_order, flat_slope, (((0,), (0,)), ((), ())), preferred_element_type=jnp.float32
        ).reshape(stacks, cores, unit, hidden)
        summed = lax.dynamic_index_in_dim(full, core_pos, 1, False)
        for shift in range(1, cores):
            side = lax.dynamic_index_in_dim(full, (core_pos + shift) % cores, 1, False)
            turn = [(i, (i + shift) % cores) for i in range(cores)]
            came = lax.ppermute(side.astype(jnp.bfloat16), "core", turn)
            summed = summed + came.astype(jnp.float32)
        weight_grad = exchange(summed, ("far", "near")) * grad_scale

    table = exchange(table, "section")
    table = table.reshape(fars, slot_count, TROWS // sections, emb_width)
    table_grad = exchange(table, "far")
    table_grad = table_grad * grad_scale
    return (weight_grad[None], table_grad)


def solution(mesh):
    sections, owners = mesh.devices.shape
    cores = 2 if owners % 2 == 0 else 1
    stacks = owners // cores
    nears = 2 if stacks % 2 == 0 else 1
    inner = Mesh(
        mesh.devices.reshape(sections, stacks // nears, nears, cores),
        ("section", "far", "near", "core"),
    )
    own = ("far", "near", "core")

    return jax.shard_map(
        per_device,
        mesh=inner,
        in_specs=(
            P("section", None, None),
            P("section", None, own, None),
            P("section", None, own, None),
            P(None, own, None),
            P(None, own + ("section",), None, None),
            P(None, own + ("section",), None),
        ),
        out_specs=(P("section", own, None), P(own, "section", None)),
        check_vma=False,
    )
```

```python
import functools
import math

import jax
import jax.numpy as jnp
from jax import lax
from jax.experimental import pallas as pl
from jax.experimental.pallas import tpu as pltpu
from jax.sharding import Mesh, PartitionSpec as P


TROWS = 512
STREAMS = 2
GROUPS = 2
NEAR_SLOTS = 4


def pair_body(where_ref, *rest, features, per_far, group_size, row_split, marks):
    piece_refs, emb_ref = rest[: len(marks)], rest[len(marks)]
    out_refs, held = rest[len(marks) + 1 : -1], rest[-1]
    flat = piece_refs[0][...]
    for mark, ref in zip(marks[1:], piece_refs[1:]):
        flat = jnp.where(where_ref[0] == mark, ref[...], flat)
    square = flat.reshape(flat.shape[0], features, features).astype(jnp.float32)
    both = (square + jnp.swapaxes(square, 1, 2)).astype(jnp.bfloat16)
    grads = lax.dot_general(
        both, emb_ref[0], (((2,), (1,)), ((0,), (0,))), preferred_element_type=jnp.float32
    ).astype(jnp.bfloat16)
    held[...] = jnp.swapaxes(grads, 0, 1)
    for turn, out_ref in enumerate(out_refs):
        for place in range(out_ref.shape[0]):
            far, rest_of = place // per_far, place % per_far
            slot = (far * group_size + where_ref[1 + turn]) * per_far + rest_of
            out_ref[place] = held[lax.div(slot, row_split)]


def pair_grads(where, pieces, marks, embeddings, group, slots, per_far, group_size, row_split):
    _, rows, features, emb_width = embeddings.shape
    samples, hidden = pieces[0].shape
    steps = samples // rows
    count = slots // group_size
    shape = jax.ShapeDtypeStruct((count, samples, emb_width), jnp.bfloat16)
    grid_spec = pltpu.PrefetchScalarGridSpec(
        num_scalar_prefetch=1,
        grid=(steps,),
        in_specs=[pl.BlockSpec((rows, hidden), lambda i, where: (i, 0))] * len(pieces)
        + [
            pl.BlockSpec(
                (1, rows, features, emb_width), lambda i, where: (group * steps + i, 0, 0, 0)
            )
        ],
        out_specs=[pl.BlockSpec((count, rows, emb_width), lambda i, where: (0, i, 0))]
        * group_size,
        scratch_shapes=[pltpu.VMEM((features, rows, emb_width), jnp.bfloat16)],
    )
    return pl.pallas_call(
        functools.partial(
            pair_body,
            features=features,
            per_far=per_far,
            group_size=group_size,
            row_split=row_split,
            marks=marks,
        ),
        grid_spec=grid_spec,
        out_shape=[shape] * group_size,
        compiler_params=pltpu.CompilerParams(vmem_limit_bytes=24 * 2**20),
        cost_estimate=pl.CostEstimate(
            flops=16 * samples * features * features * emb_width,
            bytes_accessed=samples * (features * emb_width * 4 + hidden * 8),
            transcendentals=0,
        ),
        name="pair_grads",
    )(where, *pieces, embeddings)


def row_sums_body(ids_ref, *rest, rows):
    arrived_refs, out_ref = rest[:-1], rest[-1]
    width = arrived_refs[0].shape[1]
    sources = len(arrived_refs)
    step = 2 if sources % 2 == 0 else 1
    positions = lax.broadcasted_iota(jnp.int32, (rows, step * width), 0)
    total = None
    for source in range(0, sources, step):
        places = ids_ref[0, :, source * width : (source + step) * width]
        left = jnp.where(positions == places, 1.0, 0.0).astype(jnp.bfloat16)
        right = jnp.concatenate([arrived_refs[source + i][0] for i in range(step)], axis=0)
        part = jnp.dot(left, right, preferred_element_type=jnp.float32)
        total = part if total is None else total + part
    out_ref[:, 0] = total.astype(out_ref.dtype).reshape(out_ref.shape[0], -1, total.shape[1])


def row_sums(ids, arrived, rows, parts):
    slots, width, emb = arrived[0].shape
    sources = len(arrived)
    in_specs = [pl.BlockSpec((1, 1, sources * width), lambda s: (s, 0, 0))]
    in_specs += [pl.BlockSpec((1, width, emb), lambda s: (s, 0, 0))] * sources
    return pl.pallas_call(
        functools.partial(row_sums_body, rows=rows),
        grid=(slots,),
        in_specs=in_specs,
        out_specs=pl.BlockSpec((parts, 1, rows // parts, emb), lambda s: (0, s, 0, 0)),
        out_shape=jax.ShapeDtypeStruct((parts, slots, rows // parts, emb), jnp.bfloat16),
        compiler_params=pltpu.CompilerParams(vmem_limit_bytes=16 * 2**20),
        cost_estimate=pl.CostEstimate(
            flops=2 * slots * rows * sources * width * emb,
            bytes_accessed=sources * slots * width * emb * 2 + slots * rows * emb * 2,
            transcendentals=0,
        ),
        name="row_sums",
    )(ids, *arrived)


def flip_body(in_ref, out_ref):
    block = in_ref[0, :, 0]
    out_ref[...] = block.reshape(-1, block.shape[-1]).T


def flip(layer_in):
    groups, in_group, sections, rows, hidden = layer_in.shape
    chunk_count = groups * sections
    return pl.pallas_call(
        flip_body,
        grid=(chunk_count,),
        in_specs=[
            pl.BlockSpec(
                (1, in_group, 1, rows, hidden),
                lambda c: (c % groups, 0, sections - 1 - c // groups, 0, 0),
            )
        ],
        out_specs=pl.BlockSpec((hidden, in_group * rows), lambda c: (0, c)),
        out_shape=jax.ShapeDtypeStruct(
            (hidden, chunk_count * in_group * rows), layer_in.dtype
        ),
        cost_estimate=pl.CostEstimate(
            flops=2 * layer_in.size * 256, bytes_accessed=layer_in.size * 4, transcendentals=0
        ),
        compiler_params=pltpu.CompilerParams(vmem_limit_bytes=16 * 2**20),
        name="flip",
    )(layer_in)


def weight_half_body(where_ref, flipped_ref, *rest, slots, far_slots, shifts, spots, merged):
    slope_refs = rest[:slots]
    came_ref = rest[slots] if merged else None
    out_refs, left, held, sems = rest[slots + merged : -3], rest[-3], rest[-2], rest[-1]
    section = where_ref[0]
    chunk_count = held.shape[0]
    stacks, unit, _ = left.shape
    blocks = []
    for turn in range(stacks):
        stack = spots(where_ref[2], turn)
        row = pl.multiple_of((stack * where_ref[3] + where_ref[1]) * unit, unit)
        blocks.append(
            pltpu.make_async_copy(
                flipped_ref.at[pl.ds(row, unit), :], left.at[turn], sems.at[chunk_count + turn]
            )
        )
    for copy in blocks:
        copy.start()
    for pos, shift in enumerate(shifts):

        @pl.when(section == pos)
        def _():
            copies = [
                pltpu.make_async_copy(slope_refs[chunk + shift], held.at[chunk], sems.at[chunk])
                for chunk in range(chunk_count)
                if chunk + shift < far_slots
            ]
            for copy in copies:
                copy.start()
            for chunk in range(len(copies), chunk_count):
                held[chunk] = slope_refs[chunk + shift][...]
            for copy in copies:
                copy.wait()

    for copy in blocks:
        copy.wait()
    right = held[...].reshape(left.shape[2], -1)
    total = jnp.dot(
        left[...].reshape(stacks * unit, -1), right, preferred_element_type=jnp.float32
    )
    if merged:
        parts = []
        for turn in range(stacks):
            row = pl.multiple_of(spots(where_ref[2], turn) * unit, unit)
            parts.append(came_ref[pl.ds(row, unit), :].astype(jnp.float32))
        total = total + jnp.concatenate(parts, axis=0)
    done = 0
    for out_ref in out_refs:
        rows = out_ref.shape[0]
        out_ref[...] = total[done : done + rows].astype(out_ref.dtype)
        done += rows


def weight_half(where, flipped, slopes, shifts, stacks, spots, came=None):
    hidden = slopes[0].shape[1]
    chunk_rows = slopes[0].shape[0]
    chunk_count = flipped.shape[1] // chunk_rows
    rows = flipped.shape[0] // 2
    unit = rows // stacks
    far_slots = len(slopes) - NEAR_SLOTS
    in_specs = [pl.BlockSpec(memory_space=pl.ANY)] * (1 + far_slots)
    in_specs += [pl.BlockSpec(memory_space=pltpu.VMEM)] * NEAR_SLOTS
    args = [flipped] + list(slopes)
    if came is None:
        shapes = [jax.ShapeDtypeStruct((rows, hidden), jnp.bfloat16)]
    else:
        in_specs.append(pl.BlockSpec(came.shape, lambda i, where: (0, 0)))
        args.append(came)
        shapes = [
            jax.ShapeDtypeStruct((unit, hidden), jnp.float32),
            jax.ShapeDtypeStruct((unit, hidden), jnp.float32),
            jax.ShapeDtypeStruct((2 * unit, hidden), jnp.bfloat16),
        ]
    grid_spec = pltpu.PrefetchScalarGridSpec(
        num_scalar_prefetch=1,
        grid=(1,),
        in_specs=in_specs,
        out_specs=[pl.BlockSpec(shape.shape, lambda i, where: (0, 0)) for shape in shapes],
        scratch_shapes=[
            pltpu.VMEM((stacks, unit, flipped.shape[1]), jnp.bfloat16),
            pltpu.VMEM((chunk_count, chunk_rows, hidden), jnp.bfloat16),
            pltpu.SemaphoreType.DMA((chunk_count + stacks,)),
        ],
    )
    return pl.pallas_call(
        functools.partial(
            weight_half_body,
            slots=len(slopes),
            far_slots=far_slots,
            shifts=shifts,
            spots=spots,
            merged=came is not None,
        ),
        grid_spec=grid_spec,
        out_shape=shapes,
        compiler_params=pltpu.CompilerParams(vmem_limit_bytes=24 * 2**20),
        cost_estimate=pl.CostEstimate(
            flops=flipped.size * hidden, bytes_accessed=flipped.size * 6, transcendentals=0
        ),
        name="weight_half",
    )(where, *args)


def natural(stack, turn):
    return turn


def from_own(stack, turn):
    return ((stack // 2) ^ (turn % 2)) * 2 + ((stack % 2) ^ (turn // 2))


def exchange(blocks, axis):
    size = lax.axis_size(axis)
    place = lax.axis_index(axis)
    if size > 8:
        came = lax.all_to_all(
            blocks.astype(jnp.bfloat16), axis, split_axis=0, concat_axis=0, tiled=True
        )
        return jnp.sum(came.astype(jnp.float32), axis=0)
    total = lax.dynamic_index_in_dim(blocks, place, 0, False).astype(jnp.float32)
    for shift in range(1, size):
        sent = lax.dynamic_index_in_dim(blocks, (place + shift) % size, 0, False)
        turn = [(i, (i + shift) % size) for i in range(size)]
        came = lax.ppermute(sent.astype(jnp.bfloat16), axis, turn)
        total = total + came.astype(jnp.float32)
    return total


def links_at(slot, sections):
    last = sections - 1
    chunk_count = GROUPS * sections
    pairs = []
    for section in range(1, sections):
        if 0 <= slot - STREAMS * (last - section) < chunk_count:
            pairs.append((section, section - 1))
    chunk = slot - STREAMS * last
    if 0 <= chunk and last - chunk // GROUPS > 0:
        pairs.append((0, last - chunk // GROUPS))
    return pairs


def after(value, *others):
    return lax.optimization_barrier((value,) + others)[0]


def per_device(weights, inputs, preact, cotangent, embeddings, row_ids):
    sections = lax.axis_size("section")
    fars = lax.axis_size("far")
    nears = lax.axis_size("near")
    stacks = fars * nears
    cores = lax.axis_size("core")
    owners = stacks * cores
    section_pos = lax.axis_index("section")
    core_pos = lax.axis_index("core")
    stack_pos = lax.axis_index("far") * nears + lax.axis_index("near")
    micro_count, batch_rows, hidden = cotangent.shape
    features = embeddings.shape[2]
    emb_width = embeddings.shape[3]
    quarter = batch_rows // sections
    row_split = max(1, owners // features)
    slot_count = features * row_split // owners
    grad_scale = 1.0 / math.sqrt(micro_count * batch_rows * owners)
    last = sections - 1
    is_last = section_pos == last
    layer_w = weights[0]

    in_group = micro_count // GROUPS
    chunk_count = GROUPS * sections
    chunk_rows = in_group * quarter
    view = (GROUPS, in_group, sections, quarter, hidden)
    cot_view = cotangent.reshape(view)
    pre_view = preact[0].reshape(view)

    fill = STREAMS * last
    total_slots = chunk_count + fill
    shifts = [STREAMS * (last - pos) for pos in range(sections)]
    shift_now = STREAMS * (last - section_pos)
    unit = hidden // owners
    in_view = inputs[0].reshape(view)
    flipped = None
    group_size = nears * cores
    near_core = lax.axis_index("near") * cores + core_pos
    held_slots = (
        jnp.arange(fars, dtype=jnp.int32)[:, None] * (group_size * slot_count)
        + near_core * slot_count
        + jnp.arange(slot_count, dtype=jnp.int32)[None, :]
    ).reshape(fars * slot_count)

    partners = [near_core]
    ways = [None]
    for turn in range(1, group_size):
        flip_near, flip_core = turn // cores, turn % cores
        near, core = near_core // cores, near_core % cores
        partners.append((near ^ flip_near) * cores + (core ^ flip_core))
        ways.append(
            [
                (i, (i // cores ^ flip_near) * cores + (i % cores ^ flip_core))
                for i in range(group_size)
            ]
        )

    def to_holders(blocks):
        came = [blocks[0]]
        for turn in range(1, group_size):
            came.append(lax.ppermute(blocks[turn], ("near", "core"), ways[turn]))
        return came

    received = {}
    slopes = []
    arrived = []
    ids = None
    for slot in range(total_slots):
        spot = jnp.clip(slot - shift_now, 0, chunk_count - 1)
        zero = jnp.zeros_like(spot)
        if slot >= 2 * STREAMS and slot % STREAMS == 0:
            pre_view = after(pre_view, passed)
        pre_now = lax.dynamic_slice(
            pre_view,
            (lax.rem(spot, GROUPS), zero, last - lax.div(spot, GROUPS), zero, zero),
            (1, in_group, 1, quarter, hidden),
        ).reshape(chunk_rows, hidden)
        if slot < chunk_count:
            incoming = cot_view[slot % GROUPS, :, last - slot // GROUPS]
            incoming = incoming.reshape(chunk_rows, hidden)
            if slot >= STREAMS:
                incoming = jnp.where(is_last, incoming, received[slot - STREAMS])
        else:
            incoming = received[slot - STREAMS]
        slope = jnp.where(pre_now > 0, incoming, jnp.zeros_like(incoming))
        slopes.append(slope)
        passed = lax.dot_general(
            slope, layer_w, (((1,), (1,)), ((), ())), preferred_element_type=jnp.float32
        ).astype(jnp.bfloat16)
        pairs = links_at(slot, sections)
        if pairs:
            received[slot] = lax.ppermute(passed, "section", pairs)
        if slot == 2 * STREAMS - 1:
            ids = jnp.transpose(after(row_ids, passed), (2, 0, 1))
            ids = jnp.repeat(ids.reshape(features, micro_count * quarter), row_split, axis=0)
            ids = ids.reshape(fars, group_size, slot_count, micro_count * quarter)
            ids = [
                lax.dynamic_index_in_dim(ids, partner, 1, False).reshape(
                    fars * slot_count, micro_count * quarter
                )
                for partner in partners
            ]
            ids = to_holders(ids)
            ids = jnp.concatenate(
                [
                    source[:, group * chunk_rows : (group + 1) * chunk_rows]
                    for group in range(GROUPS)
                    for source in ids
                ],
                axis=1,
            )
            if row_split > 1:
                ids = ids - ((held_slots % row_split) * TROWS)[:, None]
            ids = ids[:, None, :]
        if slot == 3 * STREAMS - 1 and unit % 128 == 0 and fars == nears == cores == 2:
            flipped = flip(after(in_view, passed))
        group = slot - (total_slots - GROUPS)
        if group < 0:
            continue
        pieces = [received[fill + GROUPS * (last - q) + group] for q in range(last, 0, -1)]
        where = jnp.stack([section_pos] + partners).astype(jnp.int32)
        blocks = pair_grads(
            where,
            pieces + [passed],
            list(range(last, -1, -1)),
            embeddings,
            group,
            features * row_split,
            slot_count,
            group_size,
            row_split,
        )
        arrived.append(to_holders(blocks))

    if flipped is not None:
        where = jnp.stack(
            [section_pos, 1 - core_pos, stack_pos, jnp.full_like(section_pos, cores)]
        ).astype(jnp.int32)
        (side,) = weight_half(where, flipped, slopes, shifts, stacks, natural)
        came = lax.ppermute(side, "core", [(0, 1), (1, 0)])
        where = jnp.stack(
            [section_pos, core_pos, stack_pos, jnp.full_like(section_pos, cores)]
        ).astype(jnp.int32)
        own_rows, far_rows, near_rows = weight_half(
            where, flipped, slopes, shifts, stacks, from_own, came
        )
        near_came = lax.ppermute(near_rows, "near", [(0, 1), (1, 0)]).astype(jnp.float32)
    table = row_sums(ids, [block for group in arrived for block in group], TROWS, sections)

    if flipped is not None:
        far_sum = (far_rows + near_came[unit:]).astype(jnp.bfloat16)
        far_came = lax.ppermute(far_sum, "far", [(0, 1), (1, 0)]).astype(jnp.float32)
        weight_grad = ((own_rows + near_came[:unit] + far_came) * grad_scale)[None]
    else:
        line = jnp.concatenate(slopes, 0)
        flat_slope = lax.dynamic_slice_in_dim(
            line,
            STREAMS * (last - section_pos) * chunk_rows,
            micro_count * batch_rows,
            0,
        )
        in_order = jnp.transpose(in_view[:, :, ::-1], (2, 0, 1, 3, 4))
        in_order = in_order.reshape(micro_count * batch_rows, hidden)
        full = lax.dot_general(
            in_order, flat_slope, (((0,), (0,)), ((), ())), preferred_element_type=jnp.float32
        ).reshape(stacks, cores, unit, hidden)
        summed = lax.dynamic_index_in_dim(full, core_pos, 1, False)
        for shift in range(1, cores):
            side = lax.dynamic_index_in_dim(full, (core_pos + shift) % cores, 1, False)
            turn = [(i, (i + shift) % cores) for i in range(cores)]
            came = lax.ppermute(side.astype(jnp.bfloat16), "core", turn)
            summed = summed + came.astype(jnp.float32)
        weight_grad = (exchange(summed, ("far", "near")) * grad_scale)[None]

    table = exchange(table, "section")
    table = table.reshape(fars, slot_count, TROWS // sections, emb_width)
    table_grad = exchange(table, "far")
    table_grad = table_grad * grad_scale
    return (weight_grad, table_grad)


def solution(mesh):
    sections, owners = mesh.devices.shape
    cores = 2 if owners % 2 == 0 else 1
    stacks = owners // cores
    nears = 2 if stacks % 2 == 0 else 1
    inner = Mesh(
        mesh.devices.reshape(sections, stacks // nears, nears, cores),
        ("section", "far", "near", "core"),
    )
    own = ("far", "near", "core")

    return jax.shard_map(
        per_device,
        mesh=inner,
        in_specs=(
            P("section", None, None),
            P("section", None, own, None),
            P("section", None, own, None),
            P(None, own, None),
            P(None, own + ("section",), None, None),
            P(None, own + ("section",), None),
        ),
        out_specs=(P("section", own, None), P(own, "section", None)),
        check_vma=False,
    )
```

```python
import functools
import math

import jax
import jax.numpy as jnp
from jax import lax
from jax.experimental import pallas as pl
from jax.experimental.pallas import tpu as pltpu
from jax.sharding import Mesh, PartitionSpec as P


TROWS = 512
STREAMS = 2
GROUPS = 2
NEAR_SLOTS = 4


def pair_body(where_ref, *rest, features, per_far, group_size, row_split, marks):
    piece_refs, emb_ref = rest[: len(marks)], rest[len(marks)]
    out_refs, held = rest[len(marks) + 1 : -1], rest[-1]
    flat = piece_refs[0][...]
    for mark, ref in zip(marks[1:], piece_refs[1:]):
        flat = jnp.where(where_ref[0] == mark, ref[...], flat)
    square = flat.reshape(flat.shape[0], features, features).astype(jnp.float32)
    both = (square + jnp.swapaxes(square, 1, 2)).astype(jnp.bfloat16)
    grads = lax.dot_general(
        both, emb_ref[0], (((2,), (1,)), ((0,), (0,))), preferred_element_type=jnp.float32
    ).astype(jnp.bfloat16)
    held[...] = jnp.swapaxes(grads, 0, 1)
    for turn, out_ref in enumerate(out_refs):
        for place in range(out_ref.shape[0]):
            far, rest_of = place // per_far, place % per_far
            slot = (far * group_size + where_ref[1 + turn]) * per_far + rest_of
            out_ref[place] = held[lax.div(slot, row_split)]


def pair_grads(where, pieces, marks, embeddings, group, slots, per_far, group_size, row_split):
    _, rows, features, emb_width = embeddings.shape
    samples, hidden = pieces[0].shape
    steps = samples // rows
    count = slots // group_size
    shape = jax.ShapeDtypeStruct((count, samples, emb_width), jnp.bfloat16)
    grid_spec = pltpu.PrefetchScalarGridSpec(
        num_scalar_prefetch=1,
        grid=(steps,),
        in_specs=[pl.BlockSpec((rows, hidden), lambda i, where: (i, 0))] * len(pieces)
        + [
            pl.BlockSpec(
                (1, rows, features, emb_width), lambda i, where: (group * steps + i, 0, 0, 0)
            )
        ],
        out_specs=[pl.BlockSpec((count, rows, emb_width), lambda i, where: (0, i, 0))]
        * group_size,
        scratch_shapes=[pltpu.VMEM((features, rows, emb_width), jnp.bfloat16)],
    )
    return pl.pallas_call(
        functools.partial(
            pair_body,
            features=features,
            per_far=per_far,
            group_size=group_size,
            row_split=row_split,
            marks=marks,
        ),
        grid_spec=grid_spec,
        out_shape=[shape] * group_size,
        compiler_params=pltpu.CompilerParams(vmem_limit_bytes=24 * 2**20),
        cost_estimate=pl.CostEstimate(
            flops=16 * samples * features * features * emb_width,
            bytes_accessed=samples * (features * emb_width * 4 + hidden * 8),
            transcendentals=0,
        ),
        name="pair_grads",
    )(where, *pieces, embeddings)


def row_sums_body(where_ref, ids_ref, *rest, rows):
    arrived_refs, out_ref = rest[:-1], rest[-1]
    width = arrived_refs[0].shape[1]
    sources = len(arrived_refs)
    step = 2 if sources % 2 == 0 else 1
    positions = lax.broadcasted_iota(jnp.int32, (rows, step * width), 0)
    total = None
    for source in range(0, sources, step):
        places = ids_ref[0, :, source * width : (source + step) * width]
        left = jnp.where(positions == places, 1.0, 0.0).astype(jnp.bfloat16)
        right = jnp.concatenate([arrived_refs[source + i][0] for i in range(step)], axis=0)
        part = jnp.dot(left, right, preferred_element_type=jnp.float32)
        total = part if total is None else total + part
    out_ref[:, 0] = total.astype(out_ref.dtype).reshape(out_ref.shape[0], -1, total.shape[1])


def row_sums(first, slots, ids, arrived, rows, parts):
    _, width, emb = arrived[0].shape
    sources = len(arrived)

    def held(s, where):
        return (where[0] + s, 0, 0)

    grid_spec = pltpu.PrefetchScalarGridSpec(
        num_scalar_prefetch=1,
        grid=(slots,),
        in_specs=[pl.BlockSpec((1, 1, sources * width), held)]
        + [pl.BlockSpec((1, width, emb), held)] * sources,
        out_specs=pl.BlockSpec((parts, 1, rows // parts, emb), lambda s, where: (0, s, 0, 0)),
    )
    return pl.pallas_call(
        functools.partial(row_sums_body, rows=rows),
        grid_spec=grid_spec,
        out_shape=jax.ShapeDtypeStruct((parts, slots, rows // parts, emb), jnp.bfloat16),
        compiler_params=pltpu.CompilerParams(vmem_limit_bytes=16 * 2**20),
        cost_estimate=pl.CostEstimate(
            flops=2 * slots * rows * sources * width * emb,
            bytes_accessed=sources * slots * width * emb * 2 + slots * rows * emb * 2,
            transcendentals=0,
        ),
        name="row_sums",
    )(jnp.reshape(first, (1,)).astype(jnp.int32), ids, *arrived)


def flip_body(in_ref, out_ref):
    block = in_ref[0, :, 0]
    out_ref[...] = block.reshape(-1, block.shape[-1]).T


def flip(layer_in):
    groups, in_group, sections, rows, hidden = layer_in.shape
    chunk_count = groups * sections
    return pl.pallas_call(
        flip_body,
        grid=(chunk_count,),
        in_specs=[
            pl.BlockSpec(
                (1, in_group, 1, rows, hidden),
                lambda c: (c % groups, 0, sections - 1 - c // groups, 0, 0),
            )
        ],
        out_specs=pl.BlockSpec((hidden, in_group * rows), lambda c: (0, c)),
        out_shape=jax.ShapeDtypeStruct(
            (hidden, chunk_count * in_group * rows), layer_in.dtype
        ),
        cost_estimate=pl.CostEstimate(
            flops=2 * layer_in.size * 256, bytes_accessed=layer_in.size * 4, transcendentals=0
        ),
        compiler_params=pltpu.CompilerParams(vmem_limit_bytes=16 * 2**20),
        name="flip",
    )(layer_in)


def weight_half_body(where_ref, flipped_ref, *rest, slots, far_slots, shifts, spots, merged):
    slope_refs = rest[:slots]
    came_ref = rest[slots] if merged else None
    out_refs, left, held, sems = rest[slots + merged : -3], rest[-3], rest[-2], rest[-1]
    section = where_ref[0]
    chunk_count = held.shape[0]
    stacks, unit, _ = left.shape
    blocks = []
    for turn in range(stacks):
        stack = spots(where_ref[2], turn)
        row = pl.multiple_of((stack * where_ref[3] + where_ref[1]) * unit, unit)
        blocks.append(
            pltpu.make_async_copy(
                flipped_ref.at[pl.ds(row, unit), :], left.at[turn], sems.at[chunk_count + turn]
            )
        )
    for copy in blocks:
        copy.start()
    for pos, shift in enumerate(shifts):

        @pl.when(section == pos)
        def _():
            copies = [
                pltpu.make_async_copy(slope_refs[chunk + shift], held.at[chunk], sems.at[chunk])
                for chunk in range(chunk_count)
                if chunk + shift < far_slots
            ]
            for copy in copies:
                copy.start()
            for chunk in range(len(copies), chunk_count):
                held[chunk] = slope_refs[chunk + shift][...]
            for copy in copies:
                copy.wait()

    for copy in blocks:
        copy.wait()
    right = held[...].reshape(left.shape[2], -1)
    total = jnp.dot(
        left[...].reshape(stacks * unit, -1), right, preferred_element_type=jnp.float32
    )
    if merged:
        parts = []
        for turn in range(stacks):
            row = pl.multiple_of(spots(where_ref[2], turn) * unit, unit)
            parts.append(came_ref[pl.ds(row, unit), :].astype(jnp.float32))
        total = total + jnp.concatenate(parts, axis=0)
    done = 0
    for out_ref in out_refs:
        rows = out_ref.shape[0]
        out_ref[...] = total[done : done + rows].astype(out_ref.dtype)
        done += rows


def weight_half(where, flipped, slopes, shifts, stacks, spots, came=None):
    hidden = slopes[0].shape[1]
    chunk_rows = slopes[0].shape[0]
    chunk_count = flipped.shape[1] // chunk_rows
    rows = flipped.shape[0] // 2
    unit = rows // stacks
    far_slots = len(slopes) - NEAR_SLOTS
    in_specs = [pl.BlockSpec(memory_space=pl.ANY)] * (1 + far_slots)
    in_specs += [pl.BlockSpec(memory_space=pltpu.VMEM)] * NEAR_SLOTS
    args = [flipped] + list(slopes)
    if came is None:
        shapes = [jax.ShapeDtypeStruct((rows, hidden), jnp.bfloat16)]
    else:
        in_specs.append(pl.BlockSpec(came.shape, lambda i, where: (0, 0)))
        args.append(came)
        shapes = [jax.ShapeDtypeStruct((unit, hidden), jnp.float32)]
        shapes += [jax.ShapeDtypeStruct((unit, hidden), jnp.bfloat16)] * (stacks - 1)
    grid_spec = pltpu.PrefetchScalarGridSpec(
        num_scalar_prefetch=1,
        grid=(1,),
        in_specs=in_specs,
        out_specs=[pl.BlockSpec(shape.shape, lambda i, where: (0, 0)) for shape in shapes],
        scratch_shapes=[
            pltpu.VMEM((stacks, unit, flipped.shape[1]), jnp.bfloat16),
            pltpu.VMEM((chunk_count, chunk_rows, hidden), jnp.bfloat16),
            pltpu.SemaphoreType.DMA((chunk_count + stacks,)),
        ],
    )
    return pl.pallas_call(
        functools.partial(
            weight_half_body,
            slots=len(slopes),
            far_slots=far_slots,
            shifts=shifts,
            spots=spots,
            merged=came is not None,
        ),
        grid_spec=grid_spec,
        out_shape=shapes,
        compiler_params=pltpu.CompilerParams(vmem_limit_bytes=24 * 2**20),
        cost_estimate=pl.CostEstimate(
            flops=flipped.size * hidden, bytes_accessed=flipped.size * 6, transcendentals=0
        ),
        name="weight_half",
    )(where, *args)


def natural(stack, turn):
    return turn


def from_own(stack, turn):
    return ((stack // 2) ^ (turn % 2)) * 2 + ((stack % 2) ^ (turn // 2))


def exchange(blocks, axis):
    size = lax.axis_size(axis)
    place = lax.axis_index(axis)
    if size > 8:
        came = lax.all_to_all(
            blocks.astype(jnp.bfloat16), axis, split_axis=0, concat_axis=0, tiled=True
        )
        return jnp.sum(came.astype(jnp.float32), axis=0)
    total = lax.dynamic_index_in_dim(blocks, place, 0, False).astype(jnp.float32)
    for shift in range(1, size):
        sent = lax.dynamic_index_in_dim(blocks, (place + shift) % size, 0, False)
        turn = [(i, (i + shift) % size) for i in range(size)]
        came = lax.ppermute(sent.astype(jnp.bfloat16), axis, turn)
        total = total + came.astype(jnp.float32)
    return total


def links_at(slot, sections):
    last = sections - 1
    chunk_count = GROUPS * sections
    pairs = []
    for section in range(1, sections):
        if 0 <= slot - STREAMS * (last - section) < chunk_count:
            pairs.append((section, section - 1))
    chunk = slot - STREAMS * last
    if 0 <= chunk and last - chunk // GROUPS > 0:
        pairs.append((0, last - chunk // GROUPS))
    return pairs


def after(value, *others):
    return lax.optimization_barrier((value,) + others)[0]


def per_device(weights, inputs, preact, cotangent, embeddings, row_ids):
    sections = lax.axis_size("section")
    fars = lax.axis_size("far")
    nears = lax.axis_size("near")
    stacks = fars * nears
    cores = lax.axis_size("core")
    owners = stacks * cores
    section_pos = lax.axis_index("section")
    core_pos = lax.axis_index("core")
    stack_pos = lax.axis_index("far") * nears + lax.axis_index("near")
    micro_count, batch_rows, hidden = cotangent.shape
    features = embeddings.shape[2]
    emb_width = embeddings.shape[3]
    quarter = batch_rows // sections
    row_split = max(1, owners // features)
    slot_count = features * row_split // owners
    grad_scale = 1.0 / math.sqrt(micro_count * batch_rows * owners)
    last = sections - 1
    is_last = section_pos == last
    layer_w = weights[0]

    in_group = micro_count // GROUPS
    chunk_count = GROUPS * sections
    chunk_rows = in_group * quarter
    view = (GROUPS, in_group, sections, quarter, hidden)
    cot_view = cotangent.reshape(view)
    pre_view = preact[0].reshape(view)

    fill = STREAMS * last
    total_slots = chunk_count + fill
    shifts = [STREAMS * (last - pos) for pos in range(sections)]
    shift_now = STREAMS * (last - section_pos)
    unit = hidden // owners
    in_view = inputs[0].reshape(view)
    flipped = None
    group_size = nears * cores
    near_core = lax.axis_index("near") * cores + core_pos
    held_slots = (
        jnp.arange(fars, dtype=jnp.int32)[:, None] * (group_size * slot_count)
        + near_core * slot_count
        + jnp.arange(slot_count, dtype=jnp.int32)[None, :]
    ).reshape(fars * slot_count)

    partners = [near_core]
    ways = [None]
    for turn in range(1, group_size):
        flip_near, flip_core = turn // cores, turn % cores
        near, core = near_core // cores, near_core % cores
        partners.append((near ^ flip_near) * cores + (core ^ flip_core))
        ways.append(
            [
                (i, (i // cores ^ flip_near) * cores + (i % cores ^ flip_core))
                for i in range(group_size)
            ]
        )

    def to_holders(blocks):
        came = [blocks[0]]
        for turn in range(1, group_size):
            came.append(lax.ppermute(blocks[turn], ("near", "core"), ways[turn]))
        return came

    received = {}
    slopes = []
    arrived = []
    for slot in range(total_slots):
        spot = jnp.clip(slot - shift_now, 0, chunk_count - 1)
        zero = jnp.zeros_like(spot)
        if slot >= 2 * STREAMS and slot % STREAMS == 0:
            pre_view = after(pre_view, passed)
        pre_now = lax.dynamic_slice(
            pre_view,
            (lax.rem(spot, GROUPS), zero, last - lax.div(spot, GROUPS), zero, zero),
            (1, in_group, 1, quarter, hidden),
        ).reshape(chunk_rows, hidden)
        if slot < chunk_count:
            incoming = cot_view[slot % GROUPS, :, last - slot // GROUPS]
            incoming = incoming.reshape(chunk_rows, hidden)
            if slot >= STREAMS:
                incoming = jnp.where(is_last, incoming, received[slot - STREAMS])
        else:
            incoming = received[slot - STREAMS]
        slope = jnp.where(pre_now > 0, incoming, jnp.zeros_like(incoming))
        slopes.append(slope)
        passed = lax.dot_general(
            slope, layer_w, (((1,), (1,)), ((), ())), preferred_element_type=jnp.float32
        ).astype(jnp.bfloat16)
        pairs = links_at(slot, sections)
        if pairs:
            received[slot] = lax.ppermute(passed, "section", pairs)
        if slot == 2 * STREAMS - 1 and unit % 128 == 0 and fars == nears == cores == 2:
            flipped = flip(after(in_view, passed))
        group = slot - (total_slots - GROUPS)
        if group < 0:
            continue
        pieces = [received[fill + GROUPS * (last - q) + group] for q in range(last, 0, -1)]
        where = jnp.stack([section_pos] + partners).astype(jnp.int32)
        blocks = pair_grads(
            where,
            pieces + [passed],
            list(range(last, -1, -1)),
            embeddings,
            group,
            features * row_split,
            slot_count,
            group_size,
            row_split,
        )
        arrived.append(to_holders(blocks))

    ids = jnp.transpose(row_ids, (2, 0, 1))
    ids = jnp.repeat(ids.reshape(features, micro_count * quarter), row_split, axis=0)
    ids = ids.reshape(fars, group_size, slot_count, micro_count * quarter)
    ids = [
        lax.dynamic_index_in_dim(ids, partner, 1, False).reshape(
            fars * slot_count, micro_count * quarter
        )
        for partner in partners
    ]
    ids = to_holders(ids)
    ids = jnp.concatenate(
        [
            source[:, group * chunk_rows : (group + 1) * chunk_rows]
            for group in range(GROUPS)
            for source in ids
        ],
        axis=1,
    )
    if row_split > 1:
        ids = ids - ((held_slots % row_split) * TROWS)[:, None]
    ids = ids[:, None, :]

    if flipped is not None:
        where = jnp.stack(
            [section_pos, 1 - core_pos, stack_pos, jnp.full_like(section_pos, cores)]
        ).astype(jnp.int32)
        (side,) = weight_half(where, flipped, slopes, shifts, stacks, natural)
        came = lax.ppermute(side, "core", [(0, 1), (1, 0)])
        where = jnp.stack(
            [section_pos, core_pos, stack_pos, jnp.full_like(section_pos, cores)]
        ).astype(jnp.int32)
        own_rows, *other_rows = weight_half(where, flipped, slopes, shifts, stacks, from_own, came)
        rows_came = []
        for turn, block in enumerate(other_rows, 1):
            way = [(i, from_own(i, turn)) for i in range(stacks)]
            rows_came.append(lax.ppermute(block, ("far", "near"), way))
    from_all = [block for group in arrived for block in group]
    far_pos = lax.axis_index("far")
    if fars == 2:
        tables = []
        for far in (1 - far_pos, far_pos):
            tables.append(row_sums(far * slot_count, slot_count, ids, from_all, TROWS, sections))
        other = exchange(tables[0], "section")
        table = exchange(tables[1], "section")
        crossed = lax.ppermute(other.astype(jnp.bfloat16), "far", [(0, 1), (1, 0)])
        table_grad = (table + crossed.astype(jnp.float32)) * grad_scale
    else:
        table = row_sums(
            jnp.zeros_like(far_pos), fars * slot_count, ids, from_all, TROWS, sections
        )
        table = exchange(table, "section")
        table = table.reshape(fars, slot_count, TROWS // sections, emb_width)
        table_grad = exchange(table, "far") * grad_scale

    if flipped is not None:
        weight_grad = own_rows
        for block in rows_came:
            weight_grad = weight_grad + block.astype(jnp.float32)
        weight_grad = (weight_grad * grad_scale)[None]
    else:
        line = jnp.concatenate(slopes, 0)
        flat_slope = lax.dynamic_slice_in_dim(
            line,
            STREAMS * (last - section_pos) * chunk_rows,
            micro_count * batch_rows,
            0,
        )
        in_order = jnp.transpose(in_view[:, :, ::-1], (2, 0, 1, 3, 4))
        in_order = in_order.reshape(micro_count * batch_rows, hidden)
        full = lax.dot_general(
            in_order, flat_slope, (((0,), (0,)), ((), ())), preferred_element_type=jnp.float32
        ).reshape(stacks, cores, unit, hidden)
        summed = lax.dynamic_index_in_dim(full, core_pos, 1, False)
        for shift in range(1, cores):
            side = lax.dynamic_index_in_dim(full, (core_pos + shift) % cores, 1, False)
            turn = [(i, (i + shift) % cores) for i in range(cores)]
            came = lax.ppermute(side.astype(jnp.bfloat16), "core", turn)
            summed = summed + came.astype(jnp.float32)
        weight_grad = (exchange(summed, ("far", "near")) * grad_scale)[None]

    return (weight_grad, table_grad)


def solution(mesh):
    sections, owners = mesh.devices.shape
    cores = 2 if owners % 2 == 0 else 1
    stacks = owners // cores
    nears = 2 if stacks % 2 == 0 else 1
    inner = Mesh(
        mesh.devices.reshape(sections, stacks // nears, nears, cores),
        ("section", "far", "near", "core"),
    )
    own = ("far", "near", "core")

    return jax.shard_map(
        per_device,
        mesh=inner,
        in_specs=(
            P("section", None, None),
            P("section", None, own, None),
            P("section", None, own, None),
            P(None, own, None),
            P(None, own + ("section",), None, None),
            P(None, own + ("section",), None),
        ),
        out_specs=(P("section", own, None), P(own, "section", None)),
        check_vma=False,
    )
```
